32 devices in a mesh: dp: 8 (over z, y), expert: 4 (over x, core).
Axes of the slice: x: 2, y: 2, z: 4, core: 2. Of those that a mesh axis runs over, the one named last changes fastest.
Arguments:
- gradients: bfloat16 [8, 128, 128, 128], P('dp', 'expert'), may hold values from -600 to 600
- owner_table: int32 [4, 32], P('expert'), may hold values from 0 to 31, as said below
- step_count: int32 [1], replicated, may hold values from 1 to 8
- master: float32 [128, 128, 128], P(('dp', 'expert')), may hold values from -0.078125 to 0.078125
- first_code: bfloat16 [128, 128, 128], P(('dp', 'expert')), may hold values from -1 to 1
- first_scale: float32 [128], P(('dp', 'expert')), may hold values from 0.1 to 1
- first_power: float32 [128], P(('dp', 'expert')), may hold values from 1 to 3
- second_code: bfloat16 [128, 128, 128], P(('dp', 'expert')), may hold values from 0.0099487305 to 1
- second_scale: float32 [128], P(('dp', 'expert')), may hold values from 0.1 to 2
- second_power: float32 [128], P(('dp', 'expert')), may hold values from 1 to 3
Outputs:
- new_master: float32 [128, 128, 128], P(('dp', 'expert'))
- new_first_code: bfloat16 [128, 128, 128], P(('dp', 'expert'))
- new_first_scale: float32 [128], P(('dp', 'expert'))
- new_first_power: float32 [128], P(('dp', 'expert'))
- new_second_code: bfloat16 [128, 128, 128], P(('dp', 'expert'))
- new_second_scale: float32 [128], P(('dp', 'expert'))
- new_second_power: float32 [128], P(('dp', 'expert'))
- weight_code: bfloat16 [128, 128, 128], P('dp')
- weight_scale: bfloat16 [128], P('dp')
The draws below stay inside these ranges and needn't reach their ends.
Inputs may be any that keep to these rules, and one draw needn't show every extreme that they name: `owner_table`: each row is a permutation of 0 to 31.
All inputs are finite; a program needn't handle non-finite values. Where the reference program divides by a largest or mean magnitude, that divisor is 1e-20 or more.
Results may differ from the reference program's by a relative error of at most 0.009.
Values may be sent and summed in bfloat16 or wider, within the bound.
A program may use at most 128 MiB of HBM per device.

```python
import math
import jax
import jax.numpy as jnp
from jax import lax

D = 6144
TILE = 128
OWN = 4
BLOCK = 32
TILES = 128


def owner_rows(key):
    block_count = TILES // BLOCK
    subkeys = jax.random.split(key, block_count)

    def permute_row(subkey):
        return jax.random.permutation(subkey, BLOCK)
    return jax.vmap(permute_row)(subkeys).astype(jnp.int32)


def draw_owner_table(key, part):
    return owner_rows(jax.random.fold_in(key, 11))


def draw_gradients(key, part):
    owner_perm = owner_rows(jax.random.fold_in(key, 11))
    block_count = TILES // BLOCK
    rank_count = BLOCK // OWN
    row_ids = jnp.arange(block_count, dtype=jnp.int32)[:, None]
    slot_of = jnp.zeros((block_count, BLOCK), jnp.int32).at[row_ids, owner_perm].set(jnp.arange(BLOCK, dtype=jnp.int32)[None, :])
    owner_rank = (slot_of // OWN).reshape(TILES).astype(jnp.float32)
    rising = 1.0 + 2.0 * owner_rank / max(rank_count - 1, 1)
    tile_gain = rising * jnp.power(10.0, jax.random.uniform(jax.random.fold_in(key, 2), (TILES,), jnp.float32))
    replica_gain = jnp.power(10.0, jax.random.uniform(jax.random.fold_in(key, 3), (rank_count, TILES), jnp.float32, -0.5, 0.5))
    full_shape = (rank_count, TILES, TILE, TILE)
    values = jnp.clip(jax.random.normal(jax.random.fold_in(key, 4), full_shape, jnp.float32), -4.0, 4.0)
    scaled = values * tile_gain[None, :, None, None] * replica_gain[:, :, None, None]
    return scaled.astype(jnp.bfloat16)


def steps_of(own_key, dims, shards, smallest, high):
    gain = 1.0
    for position, blocks in shards:
        steps = jax.random.uniform(jax.random.fold_in(jax.random.fold_in(own_key, 6), position), (blocks,), jnp.float32, smallest / len(shards), high / len(shards))
        gain = gain * jnp.repeat(jnp.exp(steps), dims[position] // blocks).reshape((-1,) + (1,) * (len(dims) - 1 - position))
    return gain


def bell_draw(rng, shape, scale, most, shards=(), held_as=jnp.bfloat16):
    values = scale * jax.random.normal(rng, shape, jnp.float32)
    if shards:
        values = values * steps_of(rng, shape, shards, -0.22, 0.18)
    return jnp.clip(values, -most, most).astype(held_as)


def setup_inputs(seed: int = 0) -> dict:
    streams_of = jax.random.split(jax.random.key(seed), 11)
    gradients = draw_gradients(jax.random.fold_in(streams_of[10], 71), 0)
    owner_table = draw_owner_table(jax.random.fold_in(streams_of[10], 71), 0)
    step_count = jax.random.randint(streams_of[2], (1,), 1, 9).astype(jnp.int32)
    master = bell_draw(streams_of[3], (TILES, TILE, TILE), D ** -0.5, 0.078125, ((0, 32),), jnp.float32)
    first_code = jnp.clip(jax.random.uniform(streams_of[4], (TILES, TILE, TILE), jnp.float32, -1.0, 1.0) * steps_of(streams_of[4], (TILES, TILE, TILE), ((0, 32),), -0.4, 0.0), -1.0, 1.0).astype(jnp.bfloat16)
    first_scale = jnp.clip(jnp.exp(math.log(1.0) - 2.3025851 * jax.random.uniform(streams_of[5], (TILES,), jnp.float32) ** steps_of(streams_of[5], (TILES,), ((0, 32),), -0.2, 0.2)), 0.1, 1.0)
    first_power = jnp.clip(1.0 + 2.0 * jax.random.uniform(streams_of[6], (TILES,), jnp.float32) ** steps_of(streams_of[6], (TILES,), ((0, 32),), -0.2, 0.2), 1.0, 3.0)
    second_code = jnp.clip(jnp.exp(math.log(1.0) - 4.61031033 * jax.random.uniform(streams_of[7], (TILES, TILE, TILE), jnp.float32) ** steps_of(streams_of[7], (TILES, TILE, TILE), ((0, 32),), -0.2, 0.2)), 0.0099487305, 1.0).astype(jnp.bfloat16)
    second_scale = jnp.clip(jnp.exp(math.log(2.0) - 2.9957323 * jax.random.uniform(streams_of[8], (TILES,), jnp.float32) ** steps_of(streams_of[8], (TILES,), ((0, 32),), -0.2, 0.2)), 0.1, 2.0)
    second_power = jnp.clip(1.0 + 2.0 * jax.random.uniform(streams_of[9], (TILES,), jnp.float32) ** steps_of(streams_of[9], (TILES,), ((0, 32),), -0.2, 0.2), 1.0, 3.0)
    return dict(gradients=gradients, owner_table=owner_table, step_count=step_count, master=master, first_code=first_code, first_scale=first_scale, first_power=first_power, second_code=second_code, second_scale=second_scale, second_power=second_power)


BETA_ONE = 0.9
BETA_TWO = 0.95
LEARN_RATE = 0.01
WEIGHT_DECAY = 0.1
CLIP_RMS = 0.5
LOG_SPAN = 4.0
EPSILON = 1e-06
ADAM_EPS = 1e-08

def decode_moment(code, scale, power):
    values = code.astype(jnp.float32)
    magnitude = jnp.power(jnp.abs(values), 1.0 / power[:, None, None])
    return scale[:, None, None] * jnp.sign(values) * magnitude

def encode_moment(values):
    absval = jnp.abs(values)
    largest = lax.optimization_barrier(jnp.max(absval, axis=(1, 2)))
    average = lax.optimization_barrier(jnp.mean(absval, axis=(1, 2)))
    power = jnp.clip(LOG_SPAN / jnp.log(1.0 + largest / (average + EPSILON)), 1.0, 3.0)
    scale = largest + EPSILON
    scaled = absval / scale[:, None, None]
    coded = (jnp.sign(values) * jnp.power(scaled, power[:, None, None])).astype(jnp.bfloat16)
    return (coded, scale, power)

def finish(owned_grad, total_sq, numel, step_count, master, first_code, first_scale, first_power, second_code, second_scale, second_power):
    clip_factor = jnp.minimum(1.0, CLIP_RMS / jnp.sqrt(total_sq / numel + EPSILON))
    grad = owned_grad * clip_factor
    first_old = decode_moment(first_code, first_scale, first_power)
    second_old = decode_moment(second_code, second_scale, second_power)
    first = BETA_ONE * first_old + (1.0 - BETA_ONE) * grad
    second = BETA_TWO * second_old + (1.0 - BETA_TWO) * grad * grad
    tcount = step_count[0].astype(jnp.float32)
    bias_one = 1.0 - jnp.power(BETA_ONE, tcount)
    bias_two = 1.0 - jnp.power(BETA_TWO, tcount)
    update = first / bias_one / (jnp.sqrt(second / bias_two) + ADAM_EPS)
    new_master = master - LEARN_RATE * (update + WEIGHT_DECAY * master)
    first_out = encode_moment(first)
    second_out = encode_moment(second)
    weight_scale = (lax.optimization_barrier(jnp.max(jnp.abs(new_master), axis=(1, 2))) + EPSILON).astype(jnp.bfloat16)
    weight_code = (new_master / weight_scale.astype(jnp.float32)[:, None, None]).astype(jnp.bfloat16)
    return (new_master, first_out, second_out, weight_code, weight_scale)

def add_replica(running, replica):
    return (running + replica.astype(jnp.float32), None)

def reference(gradients, owner_table, step_count, master, first_code, first_scale, first_power, second_code, second_scale, second_power):
    block_size = owner_table.shape[1]
    expert_count = owner_table.shape[0]
    rank_count = block_size // OWN
    summed = lax.scan(add_replica, jnp.zeros(gradients.shape[1:], jnp.float32), gradients)[0]
    rank_ids = jnp.arange(rank_count, dtype=jnp.int32)[:, None, None]
    experts = jnp.arange(expert_count, dtype=jnp.int32)[None, :, None]
    within = jnp.arange(OWN, dtype=jnp.int32)[None, None, :]
    natural = experts * block_size + owner_table[experts, rank_ids * OWN + within]
    owned_grad = jnp.take(summed, natural.reshape(-1).astype(jnp.int32), axis=0)
    total_sq = jnp.sum(summed * summed)
    numel = float(master.shape[0] * TILE * TILE)
    new_master, first_out, second_out, weight_code, weight_scale = finish(owned_grad, total_sq, numel, step_count, master, first_code, first_scale, first_power, second_code, second_scale, second_power)
    return (new_master, first_out[0], first_out[1], first_out[2], second_out[0], second_out[1], second_out[2], weight_code, weight_scale)
```

```python
import functools
import math

import jax
import jax.numpy as jnp
from jax import lax
from jax.experimental import pallas as pl
from jax.experimental.pallas import tpu as pltpu
from jax.sharding import PartitionSpec as P

BETA_ONE = 0.9
BETA_TWO = 0.95
LEARN_RATE = 0.01
WEIGHT_DECAY = 0.1
CLIP_RMS = 0.5
LOG_SPAN = 4.0
EPSILON = 1e-06
ADAM_EPS = 1e-08

MESH = pl.DeviceIdType.MESH


def flip(index, mask):
    out = index
    bit = 1
    while bit <= mask:
        if mask & bit:
            out = out + bit * (1 - 2 * ((index // bit) % 2))
        bit *= 2
    return out


def bits_of(count):
    bits = []
    bit = 1
    while bit < count:
        bits.append(bit)
        bit *= 2
    return bits


def slots_of(count):
    base, bases = 0, {}
    for bit in bits_of(count):
        bases[bit] = base
        base += count // (2 * bit)
    return bases, base


def low_bit(number):
    return number & -number


def signed_power(values, logs, power):
    magnitude = jnp.where(values == 0.0, 0.0, jnp.exp(logs * power))
    return jnp.where(values < 0.0, -magnitude, magnitude)


def tile_max(values):
    return jnp.max(jnp.max(values, axis=0, keepdims=True), axis=1, keepdims=True)


def tile_sum(values):
    return jnp.sum(jnp.sum(values, axis=0, keepdims=True), axis=1, keepdims=True)


def kernel(
    ranks,
    experts,
    own,
    numel,
    table,
    step_count,
    first_scale,
    first_power,
    second_scale,
    second_power,
    grad_hbm,
    master_hbm,
    first_hbm,
    second_hbm,
    new_master_out,
    first_out,
    second_out,
    weight_out,
    first_scale_out,
    first_power_out,
    second_scale_out,
    second_power_out,
    weight_scale_out,
    gbuf,
    sendbuf,
    recvbuf,
    acc,
    master,
    first_in,
    second_in,
    first,
    second,
    first_code,
    second_code,
    weights,
    sums_expert,
    sums_rank,
    load_sem,
    store_sem,
    send_sem,
    recv_sem,
    sum_send,
    sum_recv,
    gather_send,
    gather_recv,
    scale_send,
    scale_recv,
):
    me = lax.axis_index("dp")
    expert = lax.axis_index("expert")
    side = acc.shape[1]
    bases, _ = slots_of(ranks)

    loads = [
        pltpu.make_async_copy(grad_hbm.at[0], gbuf, load_sem.at[0]),
        pltpu.make_async_copy(first_hbm, first_in, load_sem.at[1]),
        pltpu.make_async_copy(second_hbm, second_in, load_sem.at[2]),
        pltpu.make_async_copy(master_hbm, master, load_sem.at[3]),
    ]
    loads[0].start()

    barrier = pltpu.get_barrier_semaphore()
    for r in range(1, ranks):
        pl.semaphore_signal(
            barrier, inc=1, device_id=(flip(me, r), expert), device_id_type=MESH
        )
    for r in range(1, experts):
        pl.semaphore_signal(
            barrier, inc=1, device_id=(me, flip(expert, r)), device_id_type=MESH
        )
    for load in loads[1:]:
        load.start()

    def mine(r, k):
        return gbuf[table[0, flip(me, r) * own + k]]

    def rank_copy(bit, slot, k):
        at = slot * own + k
        return pltpu.make_async_remote_copy(
            src_ref=sendbuf.at[at],
            dst_ref=recvbuf.at[at],
            send_sem=send_sem.at[slot],
            recv_sem=recv_sem.at[at],
            device_id=(flip(me, bit), expert),
            device_id_type=MESH,
        )

    loads[0].wait()
    groups = list(range(ranks // 2 - 1, -1, -1))
    for j in groups:

        def place(k, carry, j=j):
            sendbuf[(bases[1] + j) * own + k] = mine(2 * j + 1, k)
            return carry

        lax.fori_loop(0, own, place, 0)
    pl.semaphore_wait(barrier, ranks + experts - 2)
    for j in groups:
        for k in range(own):
            rank_copy(1, bases[1] + j, k).start()

    loads[1].wait()
    loads[2].wait()

    def decode(k, carry):
        one = first_in[k].astype(jnp.float32)
        one_power = 1.0 / jnp.full((1, 1), first_power[k], jnp.float32)
        first[k] = (BETA_ONE * first_scale[k]) * signed_power(
            one, jnp.log(jnp.abs(one)), one_power
        )
        two = second_in[k].astype(jnp.float32)
        two_power = 1.0 / jnp.full((1, 1), second_power[k], jnp.float32)
        second[k] = (BETA_TWO * second_scale[k]) * signed_power(
            two, jnp.log(jnp.abs(two)), two_power
        )
        return carry

    lax.fori_loop(0, own, decode, 0)

    square = jnp.zeros((8, side), jnp.float32)
    for j in groups:
        r = 2 * j

        def add(k, carry, r=r):
            total = mine(r, k).astype(jnp.float32)
            for bit in bits_of(ranks):
                if r & bit:
                    slot = bases[bit] + r // (2 * bit)
                    sendbuf[slot * own + k] = total.astype(jnp.bfloat16)
                    rank_copy(bit, slot, k).start()
                    return carry
                slot = bases[bit] + r // (2 * bit)
                rank_copy(bit, slot, k).wait_recv()
                total = total + recvbuf[slot * own + k].astype(jnp.float32)
            acc[k] = total
            return carry + jnp.sum((total * total).reshape(side // 8, 8, side), axis=0)

        square = lax.fori_loop(0, own, add, square)

    def sum_copy(buffer, at, slot, target):
        return pltpu.make_async_remote_copy(
            src_ref=buffer.at[0],
            dst_ref=buffer.at[at],
            send_sem=sum_send.at[slot],
            recv_sem=sum_recv.at[slot],
            device_id=target,
            device_id_type=MESH,
        )

    expert_sums = [
        sum_copy(sums_expert, r, r - 1, (me, flip(expert, r))) for r in range(1, experts)
    ]
    rank_sums = [
        sum_copy(sums_rank, r, experts - 2 + r, (flip(me, r), expert))
        for r in range(1, ranks)
    ]
    sums_expert[0] = jnp.sum(square, axis=0, keepdims=True)
    for copy in expert_sums:
        copy.start()
    for copy in expert_sums:
        copy.wait_recv()
    sums_rank[0] = jnp.sum(sums_expert[...], axis=0)
    for copy in rank_sums:
        copy.start()

    loads[3].wait()
    steps = jnp.full((1, side), step_count[0].astype(jnp.float32), jnp.float32)
    bias_one = (1.0 - jnp.exp(steps * math.log(BETA_ONE)))[:, :1]
    bias_two = (1.0 - jnp.exp(steps * math.log(BETA_TWO)))[:, :1]
    for copy in rank_sums:
        copy.wait_recv()
    total_sq = jnp.sum(jnp.sum(sums_rank[...], axis=0), axis=1, keepdims=True)
    clip_factor = jnp.minimum(1.0, CLIP_RMS / jnp.sqrt(total_sq / numel + EPSILON))

    def gather_copy(r, bit, k):
        at = flip(expert, r) * own + k
        slot = ((r | bit) - 1) * own + k
        return pltpu.make_async_remote_copy(
            src_ref=weights.at[at],
            dst_ref=weights.at[at],
            send_sem=gather_send.at[slot],
            recv_sem=gather_recv.at[slot],
            device_id=(me, flip(expert, bit)),
            device_id_type=MESH,
        )

    def scale_copy(r):
        at = pl.ds(expert * own, own)
        return pltpu.make_async_remote_copy(
            src_ref=weight_scale_out.at[at],
            dst_ref=weight_scale_out.at[at],
            send_sem=scale_send.at[r - 1],
            recv_sem=scale_recv.at[r - 1],
            device_id=(me, flip(expert, r)),
            device_id_type=MESH,
        )

    expert_bits = bits_of(experts)[::-1]

    def finish(k, carry):
        grad = acc[k] * clip_factor
        one = first[k] + (1.0 - BETA_ONE) * grad
        two = second[k] + (1.0 - BETA_TWO) * grad * grad
        first[k] = one
        second[k] = two
        update = one / bias_one / (jnp.sqrt(two / bias_two) + ADAM_EPS)
        old = master[k]
        new = old - LEARN_RATE * (update + WEIGHT_DECAY * old)
        master[k] = new
        scale = (tile_max(jnp.abs(new)) + EPSILON).astype(jnp.bfloat16).astype(jnp.float32)
        weights[expert * own + k] = (new / scale).astype(jnp.bfloat16)
        weight_scale_out[expert * own + k] = jnp.broadcast_to(scale, (1, side))
        for bit in expert_bits:
            gather_copy(0, bit, k).start()
        return carry

    lax.fori_loop(0, own, finish, 0)
    for r in range(1, experts):
        scale_copy(r).start()
    stores = [pltpu.make_async_copy(master, new_master_out, store_sem.at[0])]
    stores[0].start()

    def encode(values, code, scale_out, power_out, k):
        size = jnp.abs(values)
        largest = tile_max(size)
        average = tile_sum(size) * (1.0 / (side * side))
        power = jnp.clip(
            LOG_SPAN / jnp.log(1.0 + largest / (average + EPSILON)), 1.0, 3.0
        )
        scale = largest + EPSILON
        code[k] = signed_power(values, jnp.log(size / scale), power).astype(jnp.bfloat16)
        scale_out[k] = scale[0, 0]
        power_out[k] = power[0, 0]

    def encode_both(k, carry):
        encode(first[k], first_code, first_scale_out, first_power_out, k)
        encode(second[k], second_code, second_scale_out, second_power_out, k)
        return carry

    lax.fori_loop(0, own, encode_both, 0)
    stores.append(pltpu.make_async_copy(first_code, first_out, store_sem.at[1]))
    stores.append(pltpu.make_async_copy(second_code, second_out, store_sem.at[2]))
    stores[1].start()
    stores[2].start()

    order = [0]
    for bit in expert_bits:
        order = order + [r | bit for r in order]
    for r in order[1:]:
        last = low_bit(r)
        for k in range(own):
            gather_copy(r - last, last, k).wait_recv()
            for bit in expert_bits:
                if bit < last:
                    gather_copy(r, bit, k).start()
    for r in range(1, experts):
        scale_copy(r).wait_recv()
    stores.append(pltpu.make_async_copy(weights, weight_out, store_sem.at[3]))
    stores[3].start()

    for bit in bits_of(ranks):
        for j in range(ranks // (2 * bit)):
            slot = bases[bit] + j
            tiles = pl.ds(slot * own, own)
            pltpu.make_async_remote_copy(
                src_ref=sendbuf.at[tiles],
                dst_ref=recvbuf.at[tiles],
                send_sem=send_sem.at[slot],
                recv_sem=recv_sem.at[slot * own],
                device_id=(flip(me, bit), expert),
                device_id_type=MESH,
            ).wait_send()
    for copy in expert_sums + rank_sums:
        copy.wait_send()
    for r in order[1:]:
        for k in range(own):
            gather_copy(r - low_bit(r), low_bit(r), k).wait_send()
    for r in range(1, experts):
        scale_copy(r).wait_send()
    for store in stores:
        store.wait()


def on_device(
    gradients,
    owner_table,
    step_count,
    master,
    first_code,
    first_scale,
    first_power,
    second_code,
    second_scale,
    second_power,
):
    ranks, experts = lax.axis_size("dp"), lax.axis_size("expert")
    own, side = master.shape[0], master.shape[1]
    block = gradients.shape[1]
    numel = float(own * ranks * experts * side * side)
    _, slots = slots_of(ranks)
    tiles = (own, side, side)
    smem = pl.BlockSpec(memory_space=pltpu.SMEM)
    vmem = pl.BlockSpec(memory_space=pltpu.VMEM)
    hbm = pl.BlockSpec(memory_space=pl.ANY)
    small = jax.ShapeDtypeStruct((own,), jnp.float32)
    dma = pltpu.SemaphoreType.DMA
    out = pl.pallas_call(
        functools.partial(kernel, ranks, experts, own, numel),
        out_shape=(
            jax.ShapeDtypeStruct(tiles, jnp.float32),
            jax.ShapeDtypeStruct(tiles, jnp.bfloat16),
            jax.ShapeDtypeStruct(tiles, jnp.bfloat16),
            jax.ShapeDtypeStruct((experts * own, side, side), jnp.bfloat16),
            small,
            small,
            small,
            small,
            jax.ShapeDtypeStruct((experts * own, 1, side), jnp.float32),
        ),
        in_specs=[smem] * 6 + [hbm] * 4,
        out_specs=(hbm,) * 4 + (smem,) * 4 + (vmem,),
        scratch_shapes=[
            pltpu.VMEM((block, side, side), jnp.bfloat16),
            pltpu.VMEM((slots * own, side, side), jnp.bfloat16),
            pltpu.VMEM((slots * own, side, side), jnp.bfloat16),
            pltpu.VMEM(tiles, jnp.float32),
            pltpu.VMEM(tiles, jnp.float32),
            pltpu.VMEM(tiles, jnp.bfloat16),
            pltpu.VMEM(tiles, jnp.bfloat16),
            pltpu.VMEM(tiles, jnp.float32),
            pltpu.VMEM(tiles, jnp.float32),
            pltpu.VMEM(tiles, jnp.bfloat16),
            pltpu.VMEM(tiles, jnp.bfloat16),
            pltpu.VMEM((experts * own, side, side), jnp.bfloat16),
            pltpu.VMEM((experts, 1, side), jnp.float32),
            pltpu.VMEM((ranks, 1, side), jnp.float32),
            dma((4,)),
            dma((4,)),
            dma((slots,)),
            dma((slots * own,)),
            dma((experts + ranks - 2,)),
            dma((experts + ranks - 2,)),
            dma(((experts - 1) * own,)),
            dma(((experts - 1) * own,)),
            dma((experts - 1,)),
            dma((experts - 1,)),
        ],
        compiler_params=pltpu.CompilerParams(
            collective_id=0, has_side_effects=True, vmem_limit_bytes=48 << 20
        ),
    )(
        owner_table,
        step_count,
        first_scale,
        first_power,
        second_scale,
        second_power,
        gradients,
        master,
        first_code,
        second_code,
    )
    new_master, first_new, second_new, weights = out[:4]
    scales = out[8][:, 0, 0].astype(jnp.bfloat16)
    return (
        new_master,
        first_new,
        out[4],
        out[5],
        second_new,
        out[6],
        out[7],
        weights,
        scales,
    )


def solution(mesh):
    in_specs = (
        P("dp", "expert", None, None),
        P("expert", None),
        P(),
        P(("dp", "expert"), None, None),
        P(("dp", "expert"), None, None),
        P(("dp", "expert")),
        P(("dp", "expert")),
        P(("dp", "expert"), None, None),
        P(("dp", "expert")),
        P(("dp", "expert")),
    )
    out_specs = (
        P(("dp", "expert"), None, None),
        P(("dp", "expert"), None, None),
        P(("dp", "expert")),
        P(("dp", "expert")),
        P(("dp", "expert"), None, None),
        P(("dp", "expert")),
        P(("dp", "expert")),
        P("dp", None, None),
        P("dp"),
    )
    return jax.shard_map(
        on_device, mesh=mesh, in_specs=in_specs, out_specs=out_specs, check_vma=False
    )
```

```python
import functools
import math

import jax
import jax.numpy as jnp
from jax import lax
from jax.experimental import pallas as pl
from jax.experimental.pallas import tpu as pltpu
from jax.sharding import PartitionSpec as P

BETA_ONE = 0.9
BETA_TWO = 0.95
LEARN_RATE = 0.01
WEIGHT_DECAY = 0.1
CLIP_RMS = 0.5
LOG_SPAN = 4.0
EPSILON = 1e-06
ADAM_EPS = 1e-08

MESH = pl.DeviceIdType.MESH


def flip(index, mask):
    out = index
    bit = 1
    while bit <= mask:
        if mask & bit:
            out = out + bit * (1 - 2 * ((index // bit) % 2))
        bit *= 2
    return out


def bits_of(count):
    bits = []
    bit = 1
    while bit < count:
        bits.append(bit)
        bit *= 2
    return bits


def slots_of(count):
    base, bases = 0, {}
    for bit in bits_of(count):
        bases[bit] = base
        base += count // (2 * bit)
    return bases, base


def low_bit(number):
    return number & -number


def signed_power(values, logs, power):
    magnitude = jnp.where(values == 0.0, 0.0, jnp.exp(logs * power))
    return jnp.where(values < 0.0, -magnitude, magnitude)


def tile_max(values):
    return jnp.max(jnp.max(values, axis=0, keepdims=True), axis=1, keepdims=True)


def tile_sum(values):
    return jnp.sum(jnp.sum(values, axis=0, keepdims=True), axis=1, keepdims=True)


def kernel(
    ranks,
    experts,
    own,
    numel,
    table_hbm,
    step_count,
    first_scale_hbm,
    first_power_hbm,
    second_scale_hbm,
    second_power_hbm,
    grad_hbm,
    master_hbm,
    first_hbm,
    second_hbm,
    master,
    first_code,
    second_code,
    weights,
    stats_out,
    weight_scale_out,
    table,
    first_scale,
    first_power,
    second_scale,
    second_power,
    gbuf,
    sendbuf,
    recvbuf,
    acc,
    first_in,
    second_in,
    first,
    second,
    sums_expert,
    sums_rank,
    load_sem,
    send_sem,
    recv_sem,
    sum_send,
    sum_recv,
    gather_send,
    gather_recv,
    scale_send,
    scale_recv,
):
    me = lax.axis_index("dp")
    expert = lax.axis_index("expert")
    side = acc.shape[1]
    bases, _ = slots_of(ranks)

    loads = [
        pltpu.make_async_copy(grad_hbm.at[0], gbuf, load_sem.at[0]),
        pltpu.make_async_copy(first_hbm, first_in, load_sem.at[1]),
        pltpu.make_async_copy(second_hbm, second_in, load_sem.at[2]),
        pltpu.make_async_copy(master_hbm, master, load_sem.at[3]),
    ]
    scalars = [
        pltpu.make_async_copy(src, dst, load_sem.at[4 + i])
        for i, (src, dst) in enumerate(
            (
                (table_hbm, table),
                (first_scale_hbm, first_scale),
                (first_power_hbm, first_power),
                (second_scale_hbm, second_scale),
                (second_power_hbm, second_power),
            )
        )
    ]
    scalars[0].start()
    loads[0].start()

    barrier = pltpu.get_barrier_semaphore()
    for r in range(1, ranks):
        pl.semaphore_signal(
            barrier, inc=1, device_id=(flip(me, r), expert), device_id_type=MESH
        )
    for r in range(1, experts):
        pl.semaphore_signal(
            barrier, inc=1, device_id=(me, flip(expert, r)), device_id_type=MESH
        )
    for load in scalars[1:] + loads[1:]:
        load.start()

    def mine(r, k):
        return gbuf[table[0, flip(me, r) * own + k]]

    def rank_copy(bit, slot, k):
        at = slot * own + k
        return pltpu.make_async_remote_copy(
            src_ref=sendbuf.at[at],
            dst_ref=recvbuf.at[at],
            send_sem=send_sem.at[slot],
            recv_sem=recv_sem.at[at],
            device_id=(flip(me, bit), expert),
            device_id_type=MESH,
        )

    scalars[0].wait()
    loads[0].wait()
    groups = list(range(ranks // 2 - 1, -1, -1))
    for j in groups:

        def place(k, carry, j=j):
            sendbuf[(bases[1] + j) * own + k] = mine(2 * j + 1, k)
            return carry

        lax.fori_loop(0, own, place, 0)
    pl.semaphore_wait(barrier, ranks + experts - 2)
    for j in groups:
        for k in range(own):
            rank_copy(1, bases[1] + j, k).start()

    for load in scalars[1:] + loads[1:3]:
        load.wait()

    def decode(k, carry):
        one = first_in[k].astype(jnp.float32)
        one_power = 1.0 / jnp.full((1, 1), first_power[k], jnp.float32)
        first[k] = (BETA_ONE * first_scale[k]) * signed_power(
            one, jnp.log(jnp.abs(one)), one_power
        )
        two = second_in[k].astype(jnp.float32)
        two_power = 1.0 / jnp.full((1, 1), second_power[k], jnp.float32)
        second[k] = (BETA_TWO * second_scale[k]) * signed_power(
            two, jnp.log(jnp.abs(two)), two_power
        )
        return carry

    lax.fori_loop(0, own, decode, 0)

    square = jnp.zeros((8, side), jnp.float32)
    for j in groups:
        r = 2 * j

        def add(k, carry, r=r):
            total = mine(r, k).astype(jnp.float32)
            for bit in bits_of(ranks):
                if r & bit:
                    slot = bases[bit] + r // (2 * bit)
                    sendbuf[slot * own + k] = total.astype(jnp.bfloat16)
                    rank_copy(bit, slot, k).start()
                    return carry
                slot = bases[bit] + r // (2 * bit)
                rank_copy(bit, slot, k).wait_recv()
                total = total + recvbuf[slot * own + k].astype(jnp.float32)
            acc[k] = total
            return carry + jnp.sum((total * total).reshape(side // 8, 8, side), axis=0)

        square = lax.fori_loop(0, own, add, square)

    def sum_copy(buffer, at, slot, target):
        return pltpu.make_async_remote_copy(
            src_ref=buffer.at[0],
            dst_ref=buffer.at[at],
            send_sem=sum_send.at[slot],
            recv_sem=sum_recv.at[slot],
            device_id=target,
            device_id_type=MESH,
        )

    expert_sums = [
        sum_copy(sums_expert, r, r - 1, (me, flip(expert, r))) for r in range(1, experts)
    ]
    rank_sums = [
        sum_copy(sums_rank, r, experts - 2 + r, (flip(me, r), expert))
        for r in range(1, ranks)
    ]
    sums_expert[0] = jnp.sum(square, axis=0, keepdims=True)
    for copy in expert_sums:
        copy.start()
    for copy in expert_sums:
        copy.wait_recv()
    sums_rank[0] = jnp.sum(sums_expert[...], axis=0)
    for copy in rank_sums:
        copy.start()

    loads[3].wait()
    steps = jnp.full((1, side), step_count[0].astype(jnp.float32), jnp.float32)
    bias_one = (1.0 - jnp.exp(steps * math.log(BETA_ONE)))[:, :1]
    bias_two = (1.0 - jnp.exp(steps * math.log(BETA_TWO)))[:, :1]
    for copy in rank_sums:
        copy.wait_recv()
    total_sq = jnp.sum(jnp.sum(sums_rank[...], axis=0), axis=1, keepdims=True)
    clip_factor = jnp.minimum(1.0, CLIP_RMS / jnp.sqrt(total_sq / numel + EPSILON))

    def gather_copy(r, bit, k):
        at = flip(expert, r) * own + k
        slot = ((r | bit) - 1) * own + k
        return pltpu.make_async_remote_copy(
            src_ref=weights.at[at],
            dst_ref=weights.at[at],
            send_sem=gather_send.at[slot],
            recv_sem=gather_recv.at[slot],
            device_id=(me, flip(expert, bit)),
            device_id_type=MESH,
        )

    def scale_copy(r):
        at = pl.ds(expert * own, own)
        return pltpu.make_async_remote_copy(
            src_ref=weight_scale_out.at[at],
            dst_ref=weight_scale_out.at[at],
            send_sem=scale_send.at[r - 1],
            recv_sem=scale_recv.at[r - 1],
            device_id=(me, flip(expert, r)),
            device_id_type=MESH,
        )

    expert_bits = bits_of(experts)[::-1]

    def finish(k, carry):
        grad = acc[k] * clip_factor
        one = first[k] + (1.0 - BETA_ONE) * grad
        two = second[k] + (1.0 - BETA_TWO) * grad * grad
        first[k] = one
        second[k] = two
        update = one / bias_one / (jnp.sqrt(two / bias_two) + ADAM_EPS)
        old = master[k]
        new = old - LEARN_RATE * (update + WEIGHT_DECAY * old)
        master[k] = new
        scale = (tile_max(jnp.abs(new)) + EPSILON).astype(jnp.bfloat16).astype(jnp.float32)
        weights[expert * own + k] = (new / scale).astype(jnp.bfloat16)
        weight_scale_out[expert * own + k] = jnp.broadcast_to(scale, (1, side))
        for bit in expert_bits:
            gather_copy(0, bit, k).start()
        return carry

    lax.fori_loop(0, own, finish, 0)
    for r in range(1, experts):
        scale_copy(r).start()

    def encode(values, code, at, k):
        size = jnp.abs(values)
        largest = tile_max(size)
        average = tile_sum(size) * (1.0 / (side * side))
        power = jnp.clip(
            LOG_SPAN / jnp.log(1.0 + largest / (average + EPSILON)), 1.0, 3.0
        )
        scale = largest + EPSILON
        code[k] = signed_power(values, jnp.log(size / scale), power).astype(jnp.bfloat16)
        stats_out[at * own + k] = jnp.broadcast_to(scale, (1, side))
        stats_out[(at + 1) * own + k] = jnp.broadcast_to(power, (1, side))

    def encode_both(k, carry):
        encode(first[k], first_code, 0, k)
        encode(second[k], second_code, 2, k)
        return carry

    lax.fori_loop(0, own, encode_both, 0)

    order = [0]
    for bit in expert_bits:
        order = order + [r | bit for r in order]
    for r in order[1:]:
        last = low_bit(r)
        for k in range(own):
            gather_copy(r - last, last, k).wait_recv()
            for bit in expert_bits:
                if bit < last:
                    gather_copy(r, bit, k).start()
    for r in range(1, experts):
        scale_copy(r).wait_recv()

    for bit in bits_of(ranks):
        for j in range(ranks // (2 * bit)):
            slot = bases[bit] + j
            tiles = pl.ds(slot * own, own)
            pltpu.make_async_remote_copy(
                src_ref=sendbuf.at[tiles],
                dst_ref=recvbuf.at[tiles],
                send_sem=send_sem.at[slot],
                recv_sem=recv_sem.at[slot * own],
                device_id=(flip(me, bit), expert),
                device_id_type=MESH,
            ).wait_send()
    for copy in expert_sums + rank_sums:
        copy.wait_send()
    for r in order[1:]:
        for k in range(own):
            gather_copy(r - low_bit(r), low_bit(r), k).wait_send()
    for r in range(1, experts):
        scale_copy(r).wait_send()


def diagonal(rows):
    count, _, lanes = rows.shape
    rows = rows[...].reshape(count, lanes)
    at = lax.broadcasted_iota(jnp.int32, rows.shape, 0)
    lane = lax.broadcasted_iota(jnp.int32, rows.shape, 1)
    return jnp.sum(jnp.where(at == lane, rows, 0.0), axis=0)[:count]


def write_kernel(
    own,
    master,
    first_code,
    second_code,
    weights,
    stats,
    weight_scale,
    master_out,
    first_out,
    first_scale_out,
    first_power_out,
    second_out,
    second_scale_out,
    second_power_out,
    weight_out,
    weight_scale_out,
    sem,
):
    pairs = (
        (weights, weight_out),
        (master, master_out),
        (first_code, first_out),
        (second_code, second_out),
    )
    copies = [
        pltpu.make_async_copy(src, dst, sem.at[i]) for i, (src, dst) in enumerate(pairs)
    ]
    for copy in copies:
        copy.start()
    outs = (first_scale_out, first_power_out, second_scale_out, second_power_out)
    for i, out in enumerate(outs):
        out[...] = diagonal(stats.at[pl.ds(i * own, own)])
    weight_scale_out[...] = diagonal(weight_scale).astype(jnp.bfloat16)
    for copy in copies:
        copy.wait()


def on_device(
    gradients,
    owner_table,
    step_count,
    master,
    first_code,
    first_scale,
    first_power,
    second_code,
    second_scale,
    second_power,
):
    ranks, experts = lax.axis_size("dp"), lax.axis_size("expert")
    own, side = master.shape[0], master.shape[1]
    block = gradients.shape[1]
    numel = float(own * ranks * experts * side * side)
    _, slots = slots_of(ranks)
    tiles = (own, side, side)
    gathered = (experts * own, side, side)
    smem, vmem = pltpu.SMEM, pltpu.VMEM
    in_vmem = pl.BlockSpec(memory_space=vmem)
    in_hbm = pl.BlockSpec(memory_space=pltpu.HBM)
    shape = jax.ShapeDtypeStruct
    small = shape((own,), jnp.float32)

    def pin(operand):
        return pltpu.with_memory_space_constraint(operand, pltpu.HBM)

    dma = pltpu.SemaphoreType.DMA
    results = pl.pallas_call(
        functools.partial(kernel, ranks, experts, own, numel),
        out_shape=(
            vmem(tiles, jnp.float32),
            vmem(tiles, jnp.bfloat16),
            vmem(tiles, jnp.bfloat16),
            vmem(gathered, jnp.bfloat16),
            vmem((4 * own, 1, side), jnp.float32),
            vmem((experts * own, 1, side), jnp.float32),
        ),
        in_specs=[in_hbm, pl.BlockSpec(memory_space=smem)] + [in_hbm] * 8,
        out_specs=(in_vmem,) * 6,
        scratch_shapes=[
            smem(owner_table.shape, jnp.int32),
            smem((own,), jnp.float32),
            smem((own,), jnp.float32),
            smem((own,), jnp.float32),
            smem((own,), jnp.float32),
            vmem((block, side, side), jnp.bfloat16),
            vmem((slots * own, side, side), jnp.bfloat16),
            vmem((slots * own, side, side), jnp.bfloat16),
            vmem(tiles, jnp.float32),
            vmem(tiles, jnp.bfloat16),
            vmem(tiles, jnp.bfloat16),
            vmem(tiles, jnp.float32),
            vmem(tiles, jnp.float32),
            vmem((experts, 1, side), jnp.float32),
            vmem((ranks, 1, side), jnp.float32),
            dma((10,)),
            dma((slots,)),
            dma((slots * own,)),
            dma((experts + ranks - 2,)),
            dma((experts + ranks - 2,)),
            dma(((experts - 1) * own,)),
            dma(((experts - 1) * own,)),
            dma((experts - 1,)),
            dma((experts - 1,)),
        ],
        compiler_params=pltpu.CompilerParams(
            collective_id=0, has_side_effects=True, vmem_limit_bytes=48 << 20
        ),
    )(
        pin(owner_table),
        step_count,
        pin(first_scale),
        pin(first_power),
        pin(second_scale),
        pin(second_power),
        pin(gradients),
        pin(master),
        pin(first_code),
        pin(second_code),
    )
    return pl.pallas_call(
        functools.partial(write_kernel, own),
        out_shape=(
            pltpu.HBM(tiles, jnp.float32),
            pltpu.HBM(tiles, jnp.bfloat16),
            small,
            small,
            pltpu.HBM(tiles, jnp.bfloat16),
            small,
            small,
            pltpu.HBM(gathered, jnp.bfloat16),
            shape((experts * own,), jnp.bfloat16),
        ),
        in_specs=[in_vmem] * 6,
        out_specs=(
            in_hbm,
            in_hbm,
            in_vmem,
            in_vmem,
            in_hbm,
            in_vmem,
            in_vmem,
            in_hbm,
            in_vmem,
        ),
        scratch_shapes=[dma((4,))],
        compiler_params=pltpu.CompilerParams(vmem_limit_bytes=16 << 20),
    )(*results)


def solution(mesh):
    in_specs = (
        P("dp", "expert", None, None),
        P("expert", None),
        P(),
        P(("dp", "expert"), None, None),
        P(("dp", "expert"), None, None),
        P(("dp", "expert")),
        P(("dp", "expert")),
        P(("dp", "expert"), None, None),
        P(("dp", "expert")),
        P(("dp", "expert")),
    )
    out_specs = (
        P(("dp", "expert"), None, None),
        P(("dp", "expert"), None, None),
        P(("dp", "expert")),
        P(("dp", "expert")),
        P(("dp", "expert"), None, None),
        P(("dp", "expert")),
        P(("dp", "expert")),
        P("dp", None, None),
        P("dp"),
    )
    return jax.shard_map(
        on_device, mesh=mesh, in_specs=in_specs, out_specs=out_specs, check_vma=False
    )
```

```python
import functools
import math

import jax
import jax.numpy as jnp
from jax import lax
from jax.experimental import pallas as pl
from jax.experimental.pallas import tpu as pltpu
from jax.sharding import PartitionSpec as P

BETA_ONE = 0.9
BETA_TWO = 0.95
LEARN_RATE = 0.01
WEIGHT_DECAY = 0.1
CLIP_RMS = 0.5
LOG_SPAN = 4.0
EPSILON = 1e-06
ADAM_EPS = 1e-08

MESH = pl.DeviceIdType.MESH


def flip(index, mask):
    out = index
    bit = 1
    while bit <= mask:
        if mask & bit:
            out = out + bit * (1 - 2 * ((index // bit) % 2))
        bit *= 2
    return out


def bits_of(count):
    bits = []
    bit = 1
    while bit < count:
        bits.append(bit)
        bit *= 2
    return bits


def slots_of(count):
    base, bases = 0, {}
    for bit in bits_of(count):
        bases[bit] = base
        base += count // (2 * bit)
    return bases, base


def low_bit(number):
    return number & -number


def signed_power(values, logs, power):
    magnitude = jnp.where(values == 0.0, 0.0, jnp.exp(logs * power))
    return jnp.where(values < 0.0, -magnitude, magnitude)


def tile_max(values):
    return jnp.max(jnp.max(values, axis=0, keepdims=True), axis=1, keepdims=True)


def tile_sum(values):
    return jnp.sum(jnp.sum(values, axis=0, keepdims=True), axis=1, keepdims=True)


def kernel(
    ranks,
    experts,
    own,
    numel,
    table_hbm,
    step_count,
    first_scale_hbm,
    first_power_hbm,
    second_scale_hbm,
    second_power_hbm,
    grad_hbm,
    master_hbm,
    first_hbm,
    second_hbm,
    master,
    first_code,
    second_code,
    weights,
    stats_out,
    weight_scale_out,
    table,
    first_scale,
    first_power,
    second_scale,
    second_power,
    gbuf,
    sendbuf,
    recvbuf,
    acc,
    first_in,
    second_in,
    first,
    second,
    sums,
    load_sem,
    send_sem,
    recv_sem,
    sum_send,
    sum_recv,
    gather_send,
    gather_recv,
    scale_send,
    scale_recv,
):
    me = lax.axis_index("dp")
    expert = lax.axis_index("expert")
    side = acc.shape[1]
    bases, _ = slots_of(ranks)

    loads = [
        pltpu.make_async_copy(grad_hbm.at[0], gbuf, load_sem.at[0]),
        pltpu.make_async_copy(first_hbm, first_in, load_sem.at[1]),
        pltpu.make_async_copy(second_hbm, second_in, load_sem.at[2]),
        pltpu.make_async_copy(master_hbm, master, load_sem.at[3]),
    ]
    scalars = [
        pltpu.make_async_copy(src, dst, load_sem.at[4 + i])
        for i, (src, dst) in enumerate(
            (
                (table_hbm, table),
                (first_scale_hbm, first_scale),
                (first_power_hbm, first_power),
                (second_scale_hbm, second_scale),
                (second_power_hbm, second_power),
            )
        )
    ]
    scalars[0].start()
    loads[0].start()

    barrier = pltpu.get_barrier_semaphore()
    peers = [(i // experts, i % experts) for i in range(ranks * experts - 1, 0, -1)]
    for r, q in peers:
        pl.semaphore_signal(
            barrier,
            inc=1,
            device_id=(flip(me, r), flip(expert, q)),
            device_id_type=MESH,
        )
    for load in scalars[1:] + loads[1:]:
        load.start()

    def mine(r, k):
        return gbuf[table[0, flip(me, r) * own + k]]

    def rank_copy(bit, slot, k):
        at = slot * own + k
        return pltpu.make_async_remote_copy(
            src_ref=sendbuf.at[at],
            dst_ref=recvbuf.at[at],
            send_sem=send_sem.at[slot],
            recv_sem=recv_sem.at[at],
            device_id=(flip(me, bit), expert),
            device_id_type=MESH,
        )

    scalars[0].wait()
    loads[0].wait()
    groups = list(range(ranks // 2 - 1, -1, -1))
    for j in groups:

        def place(k, carry, j=j):
            sendbuf[(bases[1] + j) * own + k] = mine(2 * j + 1, k)
            return carry

        lax.fori_loop(0, own, place, 0)
    pl.semaphore_wait(barrier, len(peers))
    for j in groups:
        for k in range(own):
            rank_copy(1, bases[1] + j, k).start()

    for load in scalars[1:] + loads[1:3]:
        load.wait()

    def decode(k, carry):
        one = first_in[k].astype(jnp.float32)
        one_power = 1.0 / jnp.full((1, 1), first_power[k], jnp.float32)
        first[k] = (BETA_ONE * first_scale[k]) * signed_power(
            one, jnp.log(jnp.abs(one)), one_power
        )
        two = second_in[k].astype(jnp.float32)
        two_power = 1.0 / jnp.full((1, 1), second_power[k], jnp.float32)
        second[k] = (BETA_TWO * second_scale[k]) * signed_power(
            two, jnp.log(jnp.abs(two)), two_power
        )
        return carry

    lax.fori_loop(0, own, decode, 0)

    square = jnp.zeros((8, side), jnp.float32)
    for j in groups:
        r = 2 * j

        def add(k, carry, r=r):
            total = mine(r, k).astype(jnp.float32)
            for bit in bits_of(ranks):
                if r & bit:
                    slot = bases[bit] + r // (2 * bit)
                    sendbuf[slot * own + k] = total.astype(jnp.bfloat16)
                    rank_copy(bit, slot, k).start()
                    return carry
                slot = bases[bit] + r // (2 * bit)
                rank_copy(bit, slot, k).wait_recv()
                total = total + recvbuf[slot * own + k].astype(jnp.float32)
            acc[k] = total
            return carry + jnp.sum((total * total).reshape(side // 8, 8, side), axis=0)

        square = lax.fori_loop(0, own, add, square)

    def sum_copy(src, dst, r, q):
        return pltpu.make_async_remote_copy(
            src_ref=sums.at[src],
            dst_ref=sums.at[dst],
            send_sem=sum_send,
            recv_sem=sum_recv,
            device_id=(flip(me, r), flip(expert, q)),
            device_id_type=MESH,
        )

    sums[0] = jnp.sum(square, axis=0, keepdims=True)
    for r, q in peers:
        sum_copy(0, r * experts + q, r, q).start()
    others = pl.ds(1, len(peers))
    all_sums = sum_copy(others, others, *peers[0])

    loads[3].wait()
    steps = jnp.full((1, side), step_count[0].astype(jnp.float32), jnp.float32)
    unbias_one = (1.0 / (1.0 - jnp.exp(steps * math.log(BETA_ONE))))[:, :1]
    unbias_two = (1.0 / (1.0 - jnp.exp(steps * math.log(BETA_TWO))))[:, :1]
    all_sums.wait_recv()
    total_sq = jnp.sum(jnp.sum(sums[...], axis=0), axis=1, keepdims=True)
    clip_factor = jnp.minimum(1.0, CLIP_RMS / jnp.sqrt(total_sq / numel + EPSILON))

    def gather_copy(r, bit, k):
        at = flip(expert, r) * own + k
        slot = ((r | bit) - 1) * own + k
        return pltpu.make_async_remote_copy(
            src_ref=weights.at[at],
            dst_ref=weights.at[at],
            send_sem=gather_send.at[slot],
            recv_sem=gather_recv.at[slot],
            device_id=(me, flip(expert, bit)),
            device_id_type=MESH,
        )

    def scale_copy(r):
        at = pl.ds(expert * own, own)
        return pltpu.make_async_remote_copy(
            src_ref=weight_scale_out.at[at],
            dst_ref=weight_scale_out.at[at],
            send_sem=scale_send.at[r - 1],
            recv_sem=scale_recv.at[r - 1],
            device_id=(me, flip(expert, r)),
            device_id_type=MESH,
        )

    expert_bits = bits_of(experts)[::-1]

    largest = []
    for k in range(own):
        grad = acc[k] * clip_factor
        one = first[k] + (1.0 - BETA_ONE) * grad
        two = second[k] + (1.0 - BETA_TWO) * grad * grad
        first[k] = one
        second[k] = two
        update = (one * unbias_one) / (jnp.sqrt(two * unbias_two) + ADAM_EPS)
        old = master[k]
        new = old - LEARN_RATE * (update + WEIGHT_DECAY * old)
        master[k] = new
        largest.append(tile_max(jnp.abs(new)))
    for k in range(own):
        scale = (largest[k] + EPSILON).astype(jnp.bfloat16).astype(jnp.float32)
        weights[expert * own + k] = (master[k] * (1.0 / scale)).astype(jnp.bfloat16)
        weight_scale_out[expert * own + k] = jnp.broadcast_to(scale, (1, side))
        for bit in expert_bits:
            gather_copy(0, bit, k).start()
    for r in range(1, experts):
        scale_copy(r).start()

    moments = [(ref, code, at, k) for k in range(own)
               for ref, code, at in ((first, first_code, 0), (second, second_code, 2))]
    ranges = []
    for ref, _, at, k in moments:
        size = jnp.abs(ref[k])
        largest = tile_max(size)
        average = tile_sum(size) * (1.0 / (side * side))
        power = jnp.clip(
            LOG_SPAN / jnp.log(1.0 + largest / (average + EPSILON)), 1.0, 3.0
        )
        scale = largest + EPSILON
        stats_out[at * own + k] = jnp.broadcast_to(scale, (1, side))
        stats_out[(at + 1) * own + k] = jnp.broadcast_to(power, (1, side))
        ranges.append((1.0 / scale, power))
    for (ref, code, _, k), (shrink, power) in zip(moments, ranges):
        values = ref[k]
        logs = jnp.log(jnp.abs(values) * shrink)
        code[k] = signed_power(values, logs, power).astype(jnp.bfloat16)

    order = [0]
    for bit in expert_bits:
        order = order + [r | bit for r in order]
    for r in order[1:]:
        last = low_bit(r)
        for k in range(own):
            gather_copy(r - last, last, k).wait_recv()
            for bit in expert_bits:
                if bit < last:
                    gather_copy(r, bit, k).start()
    for r in range(1, experts):
        scale_copy(r).wait_recv()

    for bit in bits_of(ranks):
        for j in range(ranks // (2 * bit)):
            slot = bases[bit] + j
            tiles = pl.ds(slot * own, own)
            pltpu.make_async_remote_copy(
                src_ref=sendbuf.at[tiles],
                dst_ref=recvbuf.at[tiles],
                send_sem=send_sem.at[slot],
                recv_sem=recv_sem.at[slot * own],
                device_id=(flip(me, bit), expert),
                device_id_type=MESH,
            ).wait_send()
    all_sums.wait_send()
    for r in order[1:]:
        for k in range(own):
            gather_copy(r - low_bit(r), low_bit(r), k).wait_send()
    for r in range(1, experts):
        scale_copy(r).wait_send()


def diagonal(rows):
    count, _, lanes = rows.shape
    rows = rows[...].reshape(count, lanes)
    at = lax.broadcasted_iota(jnp.int32, rows.shape, 0)
    lane = lax.broadcasted_iota(jnp.int32, rows.shape, 1)
    return jnp.sum(jnp.where(at == lane, rows, 0.0), axis=0)[:count]


def write_kernel(
    own,
    master,
    first_code,
    second_code,
    weights,
    stats,
    weight_scale,
    master_out,
    first_out,
    first_scale_out,
    first_power_out,
    second_out,
    second_scale_out,
    second_power_out,
    weight_out,
    weight_scale_out,
    sem,
):
    pairs = (
        (weights, weight_out),
        (master, master_out),
        (first_code, first_out),
        (second_code, second_out),
    )
    copies = [
        pltpu.make_async_copy(src, dst, sem.at[i]) for i, (src, dst) in enumerate(pairs)
    ]
    for copy in copies:
        copy.start()
    outs = (first_scale_out, first_power_out, second_scale_out, second_power_out)
    for i, out in enumerate(outs):
        out[...] = diagonal(stats.at[pl.ds(i * own, own)])
    weight_scale_out[...] = diagonal(weight_scale).astype(jnp.bfloat16)
    for copy in copies:
        copy.wait()


def on_device(
    gradients,
    owner_table,
    step_count,
    master,
    first_code,
    first_scale,
    first_power,
    second_code,
    second_scale,
    second_power,
):
    ranks, experts = lax.axis_size("dp"), lax.axis_size("expert")
    own, side = master.shape[0], master.shape[1]
    block = gradients.shape[1]
    numel = float(own * ranks * experts * side * side)
    _, slots = slots_of(ranks)
    tiles = (own, side, side)
    gathered = (experts * own, side, side)
    smem, vmem = pltpu.SMEM, pltpu.VMEM
    in_vmem = pl.BlockSpec(memory_space=vmem)
    in_hbm = pl.BlockSpec(memory_space=pltpu.HBM)
    shape = jax.ShapeDtypeStruct
    small = shape((own,), jnp.float32)

    def pin(operand):
        return pltpu.with_memory_space_constraint(operand, pltpu.HBM)

    dma = pltpu.SemaphoreType.DMA
    results = pl.pallas_call(
        functools.partial(kernel, ranks, experts, own, numel),
        out_shape=(
            vmem(tiles, jnp.float32),
            vmem(tiles, jnp.bfloat16),
            vmem(tiles, jnp.bfloat16),
            vmem(gathered, jnp.bfloat16),
            vmem((4 * own, 1, side), jnp.float32),
            vmem((experts * own, 1, side), jnp.float32),
        ),
        in_specs=[in_hbm, pl.BlockSpec(memory_space=smem)] + [in_hbm] * 8,
        out_specs=(in_vmem,) * 6,
        scratch_shapes=[
            smem(owner_table.shape, jnp.int32),
            smem((own,), jnp.float32),
            smem((own,), jnp.float32),
            smem((own,), jnp.float32),
            smem((own,), jnp.float32),
            vmem((block, side, side), jnp.bfloat16),
            vmem((slots * own, side, side), jnp.bfloat16),
            vmem((slots * own, side, side), jnp.bfloat16),
            vmem(tiles, jnp.float32),
            vmem(tiles, jnp.bfloat16),
            vmem(tiles, jnp.bfloat16),
            vmem(tiles, jnp.float32),
            vmem(tiles, jnp.float32),
            vmem((ranks * experts, 1, side), jnp.float32),
            dma((10,)),
            dma((slots,)),
            dma((slots * own,)),
            dma,
            dma,
            dma(((experts - 1) * own,)),
            dma(((experts - 1) * own,)),
            dma((experts - 1,)),
            dma((experts - 1,)),
        ],
        compiler_params=pltpu.CompilerParams(
            collective_id=0, has_side_effects=True, vmem_limit_bytes=48 << 20
        ),
    )(
        pin(owner_table),
        step_count,
        pin(first_scale),
        pin(first_power),
        pin(second_scale),
        pin(second_power),
        pin(gradients),
        pin(master),
        pin(first_code),
        pin(second_code),
    )
    return pl.pallas_call(
        functools.partial(write_kernel, own),
        out_shape=(
            pltpu.HBM(tiles, jnp.float32),
            pltpu.HBM(tiles, jnp.bfloat16),
            small,
            small,
            pltpu.HBM(tiles, jnp.bfloat16),
            small,
            small,
            pltpu.HBM(gathered, jnp.bfloat16),
            shape((experts * own,), jnp.bfloat16),
        ),
        in_specs=[in_vmem] * 6,
        out_specs=(
            in_hbm,
            in_hbm,
            in_vmem,
            in_vmem,
            in_hbm,
            in_vmem,
            in_vmem,
            in_hbm,
            in_vmem,
        ),
        scratch_shapes=[dma((4,))],
        compiler_params=pltpu.CompilerParams(vmem_limit_bytes=16 << 20),
    )(*results)


def solution(mesh):
    in_specs = (
        P("dp", "expert", None, None),
        P("expert", None),
        P(),
        P(("dp", "expert"), None, None),
        P(("dp", "expert"), None, None),
        P(("dp", "expert")),
        P(("dp", "expert")),
        P(("dp", "expert"), None, None),
        P(("dp", "expert")),
        P(("dp", "expert")),
    )
    out_specs = (
        P(("dp", "expert"), None, None),
        P(("dp", "expert"), None, None),
        P(("dp", "expert")),
        P(("dp", "expert")),
        P(("dp", "expert"), None, None),
        P(("dp", "expert")),
        P(("dp", "expert")),
        P("dp", None, None),
        P("dp"),
    )
    return jax.shard_map(
        on_device, mesh=mesh, in_specs=in_specs, out_specs=out_specs, check_vma=False
    )
```
